32 devices in a mesh: rows: 8 (over z, y), basis: 4 (over x, core).
Axes of the slice: x: 2, y: 2, z: 4, core: 2. Of those that a mesh axis runs over, the one named last changes fastest.
Arguments:
- tiles: bfloat16 [2560, 256, 256], P(('rows', 'basis')), may hold values from 0 to 1
- tile_pairs: int32 [2560, 2], P(('rows', 'basis')), may hold values from 0 to 127, as said below
- degree: int32 [32768], P('rows'), may hold values from 848 to 5088, as said below
- start_block: float32 [32768, 128], P('rows'), may hold values from -8 to 8
- stored: float32 [16, 32768, 128], P('basis', 'rows'), may hold values from -6 to 6
Outputs:
- new_blocks: float32 [2, 32768, 128], P(None, 'rows')
- diagonal_blocks: float32 [2, 128, 128], replicated
- factors: float32 [2, 128, 128], replicated
The draws below stay inside these ranges and needn't reach their ends.
Inputs may be any that keep to these rules, and one draw needn't show every extreme that they name: `tile_pairs`: tile t has its row block among the 16 blocks 16 * (t // 320) onward, and its column block within 32 blocks before or after that range of row blocks, cyclically over 128 blocks. `degree`: positive node degrees, given as an input and not equal to A's row sums; the stored blocks are not assumed orthonormal.
All inputs are finite; a program needn't handle non-finite values.
Results may differ from the reference program's by a relative error of at most 0.00076.
Values may be sent and summed in bfloat16 or wider, within the bound.
No kernel may reach another device: no remote copies, remote signals or barrier semaphores. Data moves between devices by JAX's collectives and lax.ppermute only.
A program may use at most 128 MiB of HBM per device.

```python
import jax
import jax.numpy as jnp
from jax import lax

TILE = 256
BLK = 128
STORED = 16
ITERS = 2
REACH = 2
RB_DEV = 16
GROUP_TILES = 320
TILES = 2560
NB = 128
NODES = 32768


def draw_tile_pairs(key, part):
    first_key, second_key = jax.random.split(jax.random.fold_in(key, 11))
    owner = jnp.arange(TILES, dtype=jnp.int32) // GROUP_TILES
    row_block = owner * RB_DEV + jax.random.randint(first_key, (TILES,), 0, RB_DEV, dtype=jnp.int32)
    offset = jax.random.randint(second_key, (TILES,), -REACH * RB_DEV, (REACH + 1) * RB_DEV, dtype=jnp.int32)
    column_block = jnp.mod(owner * RB_DEV + offset, NB)
    return jnp.stack([row_block, column_block], axis=1)


def degree_values(key):
    first_key = jax.random.fold_in(key, 23)
    unit_value = max(TILE * GROUP_TILES // RB_DEV // 96, 1)
    base_value = jax.random.randint(first_key, (NODES,), 8, 17, dtype=jnp.int32)
    position = jnp.arange(NODES, dtype=jnp.int32)
    trend_value = 2 + 5 * position // NODES
    return base_value * trend_value * unit_value


def draw_degree(key, part):
    return degree_values(key)


def draw_start_block(key, part):
    unit_value = max(TILE * GROUP_TILES // RB_DEV // 96, 1)
    degree_float = degree_values(key).astype(jnp.float32)
    relative = jnp.sqrt(degree_float / (48.0 * unit_value))
    noise_key, level_key, block_key, sign_key = jax.random.split(jax.random.fold_in(key, 37), 4)
    column_sign = (2 * jax.random.randint(sign_key, (BLK,), 0, 2, dtype=jnp.int32) - 1).astype(jnp.float32)
    column_mask = (jnp.arange(BLK, dtype=jnp.int32) < max(BLK // 4, 1)).astype(jnp.float32)
    noise_part = jnp.clip(jax.random.normal(noise_key, (NODES, BLK), jnp.float32), -4.0, 4.0)
    column_level = jax.random.uniform(level_key, (BLK,), jnp.float32, 0.6, 1.4)
    block_part = jnp.clip(jax.random.normal(block_key, (NB, BLK), jnp.float32), -3.0, 3.0)
    levels = (column_level * column_sign * column_mask)[None, :] + 0.5 * block_part
    smooth = jnp.repeat(levels, TILE, axis=0)
    return jnp.clip(noise_part + relative[:, None] * smooth, -8.0, 8.0)


def steps_of(key, extent, shards, smallest, high):
    loudness = 1.0
    for axis_at, blocks in shards:
        heights = jax.random.uniform(jax.random.fold_in(jax.random.fold_in(key, 6), axis_at), (blocks,), jnp.float32, smallest / len(shards), high / len(shards))
        loudness = loudness * jnp.repeat(jnp.exp(heights), extent[axis_at] // blocks).reshape((-1,) + (1,) * (len(extent) - 1 - axis_at))
    return loudness


def normal_values(stream_key, shape, scale, most, cuts=(), held_as=jnp.bfloat16):
    loudness = steps_of(stream_key, shape, cuts, -0.22, 0.18) if cuts else 1.0
    values = jax.random.normal(stream_key, shape, jnp.float32) * scale * loudness
    return jnp.minimum(jnp.maximum(values, -most), most).astype(held_as)


def setup_inputs(seed: int = 0) -> dict:
    splits = jax.random.split(jax.random.key(seed), 6)
    tiles = jnp.clip(1.0 * jax.random.uniform(splits[0], (TILES, TILE, TILE), jnp.float32) ** steps_of(splits[0], (TILES, TILE, TILE), ((0, 32),), -0.2, 0.2), 0.0, 1.0).astype(jnp.bfloat16)
    tile_pairs = draw_tile_pairs(jax.random.fold_in(splits[5], 71), 0)
    degree = draw_degree(jax.random.fold_in(splits[5], 71), 0)
    start_block = draw_start_block(jax.random.fold_in(splits[5], 71), 0)
    stored = normal_values(splits[4], (STORED, NODES, BLK), 1.0, 6.0, ((0, 4), (1, 8)), jnp.float32)
    return dict(tiles=tiles, tile_pairs=tile_pairs, degree=degree, start_block=start_block, stored=stored)


highest = lax.Precision.HIGHEST

def reference(tiles, tile_pairs, degree, start_block, stored):
    nodes, block_width = start_block.shape
    tile_width = tiles.shape[1]
    all_blocks = nodes // tile_width
    row_scale = 1.0 / jnp.sqrt(degree.astype(jnp.float32))
    groups = tiles.shape[0] // GROUP_TILES
    tile_groups = tiles.reshape(groups, GROUP_TILES, tile_width, tile_width)
    pair_groups = tile_pairs.reshape(groups, GROUP_TILES, 2)

    def apply_graph(scaled):
        tile_grid = scaled.reshape(all_blocks, tile_width, block_width)

        def visit(total, item):
            group_tiles, group_pairs = item
            chosen = jnp.take(tile_grid, group_pairs[:, 1], axis=0).astype(jnp.float32)
            products = jnp.einsum('tij,tjc->tic', group_tiles.astype(jnp.float32), chosen, precision=highest)
            return (total.at[group_pairs[:, 0]].add(products), None)
        begin = jnp.zeros((all_blocks, tile_width, block_width), jnp.float32)
        total, _ = lax.scan(visit, begin, (tile_groups, pair_groups))
        return total.reshape(nodes, block_width)
    current = start_block
    fresh = [start_block]
    block_list, diagonal_list, factor_list = ([], [], [])
    for iteration in range(ITERS):
        scaled = (row_scale[:, None] * current).astype(jnp.bfloat16)
        image = apply_graph(scaled)
        lifted = current - row_scale[:, None] * image
        fresh_stack = jnp.stack(fresh)
        stored_coef = jnp.einsum('sri,rj->sij', stored, lifted, precision=highest) / nodes
        fresh_coef = jnp.einsum('sri,rj->sij', fresh_stack, lifted, precision=highest) / nodes
        remainder = lifted - jnp.einsum('sri,sij->rj', stored, stored_coef, precision=highest)
        remainder = remainder - jnp.einsum('sri,sij->rj', fresh_stack, fresh_coef, precision=highest)
        gram = jnp.einsum('ri,rj->ij', remainder, remainder, precision=highest) / nodes
        lower = jnp.linalg.cholesky(gram)
        current = jax.scipy.linalg.solve_triangular(lower, remainder.T, lower=True).T
        fresh.append(current)
        block_list.append(current)
        diagonal_list.append(fresh_coef[-1])
        factor_list.append(lower.T)
    return (jnp.stack(block_list), jnp.stack(diagonal_list), jnp.stack(factor_list))
```

```python
import functools

import jax
import jax.numpy as jnp
from jax import lax
from jax.experimental import pallas as pl
from jax.experimental.pallas import tpu as pltpu
from jax.sharding import PartitionSpec as P

ITERS = 2
REACH = 2
PANEL = 16
CORE_BIT = 1
CHIP_BIT = 2

f32 = jnp.float32
bf16 = jnp.bfloat16
highest = lax.Precision.HIGHEST


def cost(flops, moved):
    return pl.CostEstimate(flops=int(flops), bytes_accessed=int(moved), transcendentals=0)


def halves_of(value):
    high = value.astype(bf16)
    return high, (value - high.astype(f32)).astype(bf16)


def product(left, right):
    return jnp.dot(left, right, preferred_element_type=f32)


def tile_kernel(
    step_tiles, place, row_ref, column_ref, tiles_ref, *refs
):
    pieces = len(place) * 2
    sources = refs[:pieces]
    keep_ref, send_ref, extended, total, arrived = refs[pieces:]
    half = keep_ref.shape[0]
    tile_width = tiles_ref.shape[1]
    core = lax.rem(lax.axis_index("basis"), 2)
    step = pl.program_id(0)

    @pl.when(step == 0)
    def _():
        copies = []
        for at, source in enumerate(sources):
            side = core if at % 2 == 0 else 1 - core
            begin = pl.multiple_of(place[at // 2] * 2 * half + side * half, half)
            copies.append(
                pltpu.make_async_copy(source, extended.at[pl.ds(begin, half)], arrived.at[at])
            )
        for copy in copies:
            copy.start()
        total[...] = jnp.zeros_like(total)
        for copy in copies:
            copy.wait()

    for at in range(step_tiles):
        row = row_ref[step * step_tiles + at]
        column = column_ref[step * step_tiles + at]
        block = extended[pl.ds(pl.multiple_of(column * tile_width, tile_width), tile_width), :]
        rows = pl.ds(pl.multiple_of(row * tile_width, tile_width), tile_width)
        total[rows, :] += product(tiles_ref[at], block)

    @pl.when(step == pl.num_programs(0) - 1)
    def _():
        keep_ref[...] = total[pl.ds(pl.multiple_of(core * half, half), half), :]
        send_ref[...] = total[pl.ds(pl.multiple_of((1 - core) * half, half), half), :]


def tile_products(tiles, row_local, column_local, place, sources):
    count, tile_width, _ = tiles.shape
    half, width = sources[0].shape
    step_tiles = 8 if count % 8 == 0 else 1
    return pl.pallas_call(
        functools.partial(tile_kernel, step_tiles, place),
        grid_spec=pltpu.PrefetchScalarGridSpec(
            num_scalar_prefetch=2,
            grid=(count // step_tiles,),
            in_specs=[pl.BlockSpec((step_tiles, tile_width, tile_width), lambda i, *_: (i, 0, 0))]
            + [pl.BlockSpec(memory_space=pl.ANY)] * len(sources),
            out_specs=[pl.BlockSpec((half, width), lambda i, *_: (0, 0))] * 2,
            scratch_shapes=[
                pltpu.VMEM((len(sources) * half, width), bf16),
                pltpu.VMEM((2 * half, width), f32),
                pltpu.SemaphoreType.DMA((len(sources),)),
            ],
        ),
        out_shape=[jax.ShapeDtypeStruct((half, width), f32)] * 2,
        cost_estimate=cost(2 * tiles.size * width, tiles.size * 2),
        name="tile_products",
    )(row_local, column_local, tiles, *sources)


def coefficient_kernel(fresh_count, has_before, place_ref, lifted_ref, stored_ref, *refs):
    fresh_refs = refs[:fresh_count]
    before_ref = refs[fresh_count] if has_before else None
    out_ref, left = refs[-2:]
    width = lifted_ref.shape[1]
    group = stored_ref.shape[0]
    step = pl.program_id(0)

    def put(columns, blocks):
        joined = jnp.concatenate(blocks, axis=1) if len(blocks) > 1 else blocks[0]
        high, low = halves_of(joined)
        sums = product(left[...], high) + product(left[...], low)
        sums = sums[:width, :] + sums[width:, :]
        out_ref[:, columns] = sums + before_ref[:, columns] if has_before else sums

    @pl.when(step == 0)
    def _():
        left[...] = jnp.concatenate(halves_of(lifted_ref[...].T), axis=0)

    begin = pl.multiple_of(step * group * width, width)
    put(pl.ds(begin, group * width), [stored_ref[at] for at in range(group)])

    @pl.when(step == pl.num_programs(0) - 1)
    def _():
        first = out_ref.shape[1] - fresh_count * width
        for at in range(0, fresh_count, 2):
            refs_here = fresh_refs[at : at + 2]
            put(pl.ds(first + at * width, len(refs_here) * width), [ref[...] for ref in refs_here])


def coefficients(lifted, stored, fresh, side, before):
    rows, width = lifted.shape
    count = stored.shape[0]
    group = 2 if count % 2 == 0 else 1
    columns = (count + len(fresh)) * width
    extra = [] if before is None else [before]
    whole = pl.BlockSpec((width, columns), lambda i, at: (0, 0))
    return pl.pallas_call(
        functools.partial(coefficient_kernel, len(fresh), before is not None),
        grid_spec=pltpu.PrefetchScalarGridSpec(
            num_scalar_prefetch=1,
            grid=(count // group,),
            in_specs=[
                pl.BlockSpec((rows, width), lambda i, at: (0, 0)),
                pl.BlockSpec((group, rows, width), lambda i, at: (i, at[0], 0)),
            ]
            + [pl.BlockSpec((rows, width), lambda i, at: (at[0], 0))] * len(fresh)
            + [whole] * len(extra),
            out_specs=whole,
            scratch_shapes=[pltpu.VMEM((2 * width, rows), bf16)],
        ),
        out_shape=jax.ShapeDtypeStruct((width, columns), f32),
        cost_estimate=cost(8 * rows * width * columns, 4 * rows * columns),
        name="coefficients",
    )(side, lifted, stored, *fresh, *extra)


def correction_kernel(place_ref, stored_ref, coefficient_ref, out_ref, right):
    count, _, width = stored_ref.shape

    @pl.when(pl.program_id(0) == 0)
    def _():
        for at in range(count):
            block = coefficient_ref[:, at * width : (at + 1) * width].T
            right[at * width : (at + 1) * width, :] = jnp.concatenate(halves_of(block), axis=1)

    sums = None
    for at in range(0, count, 2):
        pair = [stored_ref[i] for i in range(at, min(at + 2, count))]
        joined = jnp.concatenate(pair, axis=1) if len(pair) == 2 else pair[0]
        high, low = halves_of(joined)
        weights = right[at * width : (at + len(pair)) * width, :]
        term = product(high, weights) + product(low, weights)
        sums = term if sums is None else sums + term
    out_ref[...] = sums[:, :width] + sums[:, width:]


def correction(stored, coefficient, side):
    count, rows, width = stored.shape
    half = rows // 2
    step_rows = min(half, 512)
    steps = half // step_rows
    return pl.pallas_call(
        correction_kernel,
        grid_spec=pltpu.PrefetchScalarGridSpec(
            num_scalar_prefetch=1,
            grid=(steps,),
            in_specs=[
                pl.BlockSpec((count, step_rows, width), lambda i, at: (0, at[0] * steps + i, 0)),
                pl.BlockSpec((width, count * width), lambda i, at: (0, 0)),
            ],
            out_specs=pl.BlockSpec((step_rows, width), lambda i, at: (i, 0)),
            scratch_shapes=[pltpu.VMEM((count * width, 2 * width), bf16)],
        ),
        out_shape=jax.ShapeDtypeStruct((half, width), f32),
        cost_estimate=cost(8 * half * width * width * count, 4 * half * width * count),
        name="correction",
    )(side, stored, coefficient)


def remainder_kernel(first_column, place_ref, lifted_ref, keep_ref, near_ref, far_ref, coefficient_ref, *refs):
    fresh_refs = refs[:-2]
    out_ref, gram_ref = refs[-2:]
    width = out_ref.shape[1]
    value = lifted_ref[...] - ((keep_ref[...] + near_ref[...]) + far_ref[...])
    for at, ref in enumerate(fresh_refs):
        begin = first_column + at * width
        block = coefficient_ref[:, begin : begin + width]
        value = value - lax.dot_general(
            ref[...], block, (((1,), (1,)), ((), ())), precision=highest, preferred_element_type=f32
        )
    out_ref[...] = value
    gram_ref[...] = jnp.dot(value.T, value, precision=highest, preferred_element_type=f32)


def remainder_part(lifted, keep, near, far, coefficient, fresh, place, first_column):
    quarter, width = far.shape
    by_chip = pl.BlockSpec((quarter, width), lambda i, at: (at[0], 0))
    by_device = pl.BlockSpec((quarter, width), lambda i, at: (at[1], 0))
    here = pl.BlockSpec((quarter, width), lambda i, at: (0, 0))
    return pl.pallas_call(
        functools.partial(remainder_kernel, first_column),
        grid_spec=pltpu.PrefetchScalarGridSpec(
            num_scalar_prefetch=1,
            grid=(1,),
            in_specs=[by_chip, by_chip, by_chip, here]
            + [pl.BlockSpec(coefficient.shape, lambda i, at: (0, 0))]
            + [by_device] * len(fresh),
            out_specs=[here, pl.BlockSpec((width, width), lambda i, at: (0, 0))],
        ),
        out_shape=[
            jax.ShapeDtypeStruct((quarter, width), f32),
            jax.ShapeDtypeStruct((width, width), f32),
        ],
        cost_estimate=cost(12 * quarter * width * width * (len(fresh) + 1), 24 * quarter * width),
        name="remainder",
    )(place, lifted, keep, near, far, coefficient, *fresh)


def factor_kernel(gram_ref, upper_ref, inverse_ref, work):
    width = gram_ref.shape[0]
    row_at = lax.broadcasted_iota(jnp.int32, (width, width), 0)
    column_at = lax.broadcasted_iota(jnp.int32, (width, width), 1)
    work[:, :width] = gram_ref[...]
    work[:, width:] = (row_at == column_at).astype(f32)
    panel_row = lax.broadcasted_iota(jnp.int32, (PANEL, width), 0)
    panel_column = lax.broadcasted_iota(jnp.int32, (PANEL, width), 1)
    for begin in range(0, width, PANEL):
        end = begin + PANEL
        left = work[begin:end, :width]
        right = work[begin:end, width:]
        columns = [
            jnp.broadcast_to(left[:, begin + at : begin + at + 1], (PANEL, width)) for at in range(PANEL)
        ]
        for at in range(PANEL):
            scale = lax.rsqrt(columns[at][at : at + 1, :])
            column = columns[at] * scale
            below = jnp.where(panel_row > at, column, 0.0)
            left_row = left[at : at + 1, :] * scale
            right_row = right[at : at + 1, :] * scale
            left = jnp.where(panel_row == at, left_row, left - below * left_row)
            right = jnp.where(panel_row == at, right_row, right - below * right_row)
            for other in range(at + 1, PANEL):
                columns[other] = columns[other] - below * column[other : other + 1, :]
        left = jnp.where(panel_column >= panel_row + begin, left, 0.0)
        upper_ref[begin:end, :] = left
        inverse_ref[begin:end, :] = right
        if end < width:
            multipliers = left.T[end:, :]
            work[end:, :] -= jnp.dot(
                multipliers,
                jnp.concatenate([left, right], axis=1),
                precision=highest,
                preferred_element_type=f32,
            )


def factor(gram):
    width = gram.shape[0]
    return pl.pallas_call(
        factor_kernel,
        out_shape=[jax.ShapeDtypeStruct((width, width), f32)] * 2,
        scratch_shapes=[pltpu.VMEM((width, 2 * width), f32)],
        cost_estimate=cost(2e8, 4 * gram.size),
        name="factor",
    )(gram)


def solve_kernel(last, place_ref, inverse_ref, *refs):
    quarters = refs[:4]
    rest, right = refs[4:-1], refs[-1]
    step = pl.program_id(0)
    width = inverse_ref.shape[0]

    @pl.when(step == 0)
    def _():
        joined = jnp.concatenate(halves_of(inverse_ref[...].T), axis=1)
        right[...] = jnp.concatenate([joined, joined], axis=0)

    for at, ref in enumerate(quarters):

        @pl.when(step == at)
        def _():
            left = jnp.concatenate(halves_of(ref[...]), axis=1)
            sums = product(left, right[...])
            value = sums[:, :width] + sums[:, width:]
            if last:
                before_refs, out_ref = rest[:-1], rest[-1]
                for i, before in enumerate(before_refs):
                    out_ref[i] = before[...]
                out_ref[len(before_refs)] = value
            else:
                scale_ref, out_ref, mine_ref, other_ref = rest
                out_ref[...] = value
                target = mine_ref if at < 2 else other_ref
                quarter = ref.shape[0]
                begin = pl.multiple_of(lax.rem(place_ref[at], 2) * quarter, quarter)
                target[pl.ds(begin, quarter), :] = (scale_ref[...] * value).astype(bf16)


def solve(inverse, quarters, place, row_scale, before):
    quarter, width = quarters[0].shape
    last = before is not None
    here = pl.BlockSpec((quarter, width), lambda i, at: (0, 0))
    placed = pl.BlockSpec((quarter, width), lambda i, at: (at[i], 0))
    half = pl.BlockSpec((2 * quarter, width), lambda i, at: (0, 0))
    rows = 4 * quarter
    if last:
        extra = before
        out_specs = pl.BlockSpec((len(before) + 1, quarter, width), lambda i, at: (0, at[i], 0))
        out_shape = jax.ShapeDtypeStruct((len(before) + 1, rows, width), f32)
    else:
        extra = [row_scale]
        out_specs = [placed, half, half]
        out_shape = [jax.ShapeDtypeStruct((rows, width), f32)] + [
            jax.ShapeDtypeStruct((2 * quarter, width), bf16)
        ] * 2
    return pl.pallas_call(
        functools.partial(solve_kernel, last),
        grid_spec=pltpu.PrefetchScalarGridSpec(
            num_scalar_prefetch=1,
            grid=(4,),
            in_specs=[pl.BlockSpec((width, width), lambda i, at: (0, 0))] + [here] * 4 + [placed] * len(extra),
            out_specs=out_specs,
            scratch_shapes=[pltpu.VMEM((2 * width, 2 * width), bf16)],
        ),
        out_shape=out_shape,
        cost_estimate=cost(8 * rows * width * width, 12 * rows * width),
        name="solve",
    )(place, inverse, *quarters, *extra)


def along_rows(value, by):
    length = lax.axis_size("rows")
    return lax.ppermute(value, "rows", [(i, (i + by) % length) for i in range(length)])


def across(value, bit):
    return lax.ppermute(value, "basis", [(i, i ^ bit) for i in range(lax.axis_size("basis"))])


def summed(value, axes):
    rows, columns = value.shape
    devices = 1
    for axis in axes:
        devices *= lax.axis_size(axis)
    if rows % devices:
        return lax.psum(value, axes)
    pieces = value.reshape(devices, rows // devices, columns)
    taken = lax.all_to_all(pieces, axes, 0, 0, tiled=True)
    piece = jnp.sum(taken, axis=0)
    spread = jnp.broadcast_to(piece[None], pieces.shape)
    return lax.all_to_all(spread, axes, 0, 0, tiled=True).reshape(rows, columns)


def local(tiles, tile_pairs, degree, start_block, stored):
    rows_count = lax.axis_size("rows")
    rows_index = lax.axis_index("rows")
    basis_index = lax.axis_index("basis")
    core, chip = lax.rem(basis_index, 2), basis_index // 2
    local_rows, width = start_block.shape
    stored_here = stored.shape[0]
    half, quarter = local_rows // 2, local_rows // 4
    blocks_here = local_rows // tiles.shape[1]
    all_nodes = local_rows * rows_count
    all_blocks = blocks_here * rows_count
    row_local = tile_pairs[:, 0] - rows_index * blocks_here
    column_local = jnp.mod(tile_pairs[:, 1] - (rows_index - REACH) * blocks_here, all_blocks)
    row_scale = jnp.broadcast_to((1.0 / jnp.sqrt(degree.astype(f32)))[:, None], start_block.shape)

    def mine(value):
        return lax.dynamic_slice_in_dim(value, core * half, half, 0)

    def other(value):
        return lax.dynamic_slice_in_dim(value, (1 - core) * half, half, 0)

    side_mine = core.reshape(1)
    side_other = (1 - core).reshape(1)
    quarter_place = jnp.stack([chip, 2 * core + chip])
    solve_place = jnp.stack(
        [2 * core + chip, 2 * core + 1 - chip, 2 * (1 - core) + chip, 2 * (1 - core) + 1 - chip]
    )
    scaled = (row_scale * start_block).astype(bf16)
    scaled_mine, scaled_other = mine(scaled), other(scaled)
    scale_mine = mine(row_scale)
    distances = [distance for distance in range(-REACH, REACH + 1) if distance]
    current = start_block
    fresh = [start_block]
    diagonal_list, factor_list = ([], [])
    for iteration in range(ITERS):
        last = iteration == ITERS - 1
        got_mine = [along_rows(scaled_mine, -distance) for distance in distances]
        got_other = [across(value, CORE_BIT) for value in got_mine]
        place = [REACH] + [distance + REACH for distance in distances]
        sources = [scaled_mine, scaled_other]
        for pair in zip(got_mine, got_other):
            sources.extend(pair)
        keep, send = tile_products(tiles, row_local, column_local, place, sources)
        chip_sum = keep + across(send, CORE_BIT)
        image = chip_sum + across(chip_sum, CHIP_BIT)
        lifted = mine(current) - scale_mine * image
        lifted_other = across(lifted, CORE_BIT)
        part = coefficients(lifted, stored, fresh, side_mine, None)
        part = coefficients(lifted_other, stored, fresh, side_other, part)
        coefficient = summed(part, ("rows",)) / all_nodes
        stored_coefficient = coefficient[:, : stored_here * width]
        term_send = correction(stored, stored_coefficient, side_other)
        near = across(term_send, CORE_BIT)
        term_keep = correction(stored, stored_coefficient, side_mine)
        far = across(
            lax.dynamic_slice_in_dim(term_keep, (1 - chip) * quarter, quarter, 0)
            + lax.dynamic_slice_in_dim(near, (1 - chip) * quarter, quarter, 0),
            CHIP_BIT,
        )
        remainder, gram_part = remainder_part(
            lifted, term_keep, near, far, coefficient, fresh, quarter_place, stored_here * width
        )
        remainder_far = across(remainder, CHIP_BIT)
        quarters = [remainder, remainder_far, across(remainder, CORE_BIT), across(remainder_far, CORE_BIT)]
        gram = summed(gram_part, ("rows", "basis")) / all_nodes
        upper, inverse = factor(gram)
        diagonal_list.append(coefficient[:, -width:].T)
        factor_list.append(upper)
        if last:
            blocks = solve(inverse, quarters, solve_place, None, fresh[1:])
        else:
            current, scaled_mine, scaled_other = solve(inverse, quarters, solve_place, row_scale, None)
            fresh.append(current)
    return (blocks, jnp.stack(diagonal_list), jnp.stack(factor_list))


def solution(mesh):
    placed = (
        P(("rows", "basis"), None, None),
        P(("rows", "basis"), None),
        P("rows"),
        P("rows", None),
        P("basis", "rows", None),
    )
    return jax.shard_map(
        local,
        mesh=mesh,
        in_specs=placed,
        out_specs=(P(None, "rows", None), P(), P()),
        check_vma=False,
    )
```

```python
import functools

import jax
import jax.numpy as jnp
from jax import lax
from jax.experimental import pallas as pl
from jax.experimental.pallas import tpu as pltpu
from jax.sharding import PartitionSpec as P

ITERS = 2
REACH = 2
PANEL = 16
CORE_BIT = 1
CHIP_BIT = 2

f32 = jnp.float32
bf16 = jnp.bfloat16
highest = lax.Precision.HIGHEST


def cost(flops, moved):
    return pl.CostEstimate(flops=int(flops), bytes_accessed=int(moved), transcendentals=0)


def halves_of(value):
    high = value.astype(bf16)
    return high, (value - high.astype(f32)).astype(bf16)


def product(left, right):
    return jnp.dot(left, right, preferred_element_type=f32)


def quarter_places():
    basis_index = lax.axis_index("basis")
    core, chip = lax.rem(basis_index, 2), basis_index // 2
    return [2 * core + chip, 2 * core + 1 - chip, 2 * (1 - core) + chip, 2 * (1 - core) + 1 - chip]


def tile_kernel(step_tiles, targets, row_ref, column_ref, tiles_ref, *refs):
    pieces = len(targets)
    sources = refs[:pieces]
    outs = refs[pieces : pieces + 2]
    extended, total, arrived = refs[pieces + 2 :]
    quarter = outs[0].shape[0] // 2
    count, tile_width, _ = tiles_ref.shape
    places = quarter_places()
    copies = []
    for source, (at, index, which) in zip(sources, targets):
        begin = pl.multiple_of((at * 4 + places[which]) * quarter, quarter)
        copies.append(
            pltpu.make_async_copy(
                source.at[pl.ds(index * quarter, quarter)],
                extended.at[pl.ds(begin, quarter)],
                arrived.at[len(copies)],
            )
        )
    for copy in copies:
        copy.start()

    total[...] = jnp.zeros_like(total)
    for copy in copies:
        copy.wait()

    def visit(step, carry):
        for at in range(step_tiles):
            tile = step * step_tiles + at
            column = pl.multiple_of(column_ref[tile] * tile_width, tile_width)
            rows = pl.ds(pl.multiple_of(row_ref[tile] * tile_width, tile_width), tile_width)
            total[rows, :] += product(tiles_ref[tile], extended[pl.ds(column, tile_width), :])
        return carry

    lax.fori_loop(0, count // step_tiles, visit, 0)
    for at, place in enumerate(places):
        begin = at % 2 * quarter
        rows = pl.ds(pl.multiple_of(place * quarter, quarter), quarter)
        outs[at // 2][begin : begin + quarter, :] = total[rows, :]


def in_vmem(count):
    return [pl.BlockSpec(memory_space=pltpu.VMEM)] * count


def limits(mib):
    return pltpu.CompilerParams(vmem_limit_bytes=mib << 20)


def tile_products(tiles, row_local, column_local, ranges, sources):
    count = tiles.shape[0]
    width = sources[0][0][0].shape[1]
    quarter = sources[0][0][0].shape[0]
    step_tiles = 8 if count % 8 == 0 else 1
    targets, arrays = [], []
    for at, sides in zip(ranges, sources):
        for side, parts in enumerate(sides):
            for which in range(2):
                index = which if len(parts) == 1 else 0
                targets.append((at, index, 2 * side + which))
                arrays.append(parts[0] if len(parts) == 1 else parts[which])
    sources = arrays
    return pl.pallas_call(
        functools.partial(tile_kernel, step_tiles, targets),
        in_specs=[pl.BlockSpec(memory_space=pltpu.SMEM)] * 2
        + in_vmem(1)
        + [pl.BlockSpec(memory_space=pltpu.HBM)] * len(sources),
        out_specs=in_vmem(2),
        scratch_shapes=[
            pltpu.VMEM((len(sources) * quarter, width), bf16),
            pltpu.VMEM((4 * quarter, width), f32),
            pltpu.SemaphoreType.DMA((len(sources),)),
        ],
        out_shape=[jax.ShapeDtypeStruct((2 * quarter, width), f32)] * 2,
        compiler_params=limits(28),
        cost_estimate=cost(2 * tiles.size * width, tiles.size * 2),
        name="tile_products",
    )(row_local, column_local, tiles, *sources)


def coefficient_kernel(which, fresh_count, has_before, lifted_ref, stored_ref, *refs):
    fresh_refs = refs[: 2 * fresh_count]
    before_ref = refs[2 * fresh_count] if has_before else None
    out_ref = refs[-1]
    width = lifted_ref.shape[1]
    quarter = lifted_ref.shape[0] // 2
    left = jnp.concatenate(halves_of(lifted_ref[...].T), axis=0)
    blocks_count = stored_ref.shape[0] + fresh_count

    def take(at, side):
        if at < stored_ref.shape[0]:
            begin = quarter_places()[which[side]] * quarter
            return stored_ref[at, pl.ds(pl.multiple_of(begin, quarter), quarter), :]
        return fresh_refs[2 * (at - stored_ref.shape[0]) + side][...]

    for at in range(0, blocks_count, 2):
        pair = range(at, min(at + 2, blocks_count))
        sums = None
        for side in range(2):
            blocks = [take(i, side) for i in pair]
            joined = jnp.concatenate(blocks, axis=1) if len(blocks) > 1 else blocks[0]
            high, low = halves_of(joined)
            part = left[:, side * quarter : (side + 1) * quarter]
            term = product(part, high) + product(part, low)
            sums = term if sums is None else sums + term
        sums = sums[:width, :] + sums[width:, :]
        columns = slice(at * width, (at + len(pair)) * width)
        out_ref[:, columns] = sums + before_ref[:, columns] if has_before else sums


def coefficients(which, lifted, stored, fresh, before):
    half, width = lifted.shape
    columns = (stored.shape[0] + len(fresh)) * width
    extra = [] if before is None else [before]
    pieces = [block[at] for block in fresh for at in which]
    return pl.pallas_call(
        functools.partial(coefficient_kernel, which, len(fresh), before is not None),
        in_specs=in_vmem(2 + len(pieces) + len(extra)),
        out_specs=in_vmem(1)[0],
        out_shape=jax.ShapeDtypeStruct((width, columns), f32),
        compiler_params=limits(24),
        cost_estimate=cost(8 * half * width * columns, 4 * half * columns),
        name="coefficients",
    )(lifted, stored, *pieces, *extra)


def correction_kernel(which, stored_ref, coefficient_ref, *outs):
    count, _, width = stored_ref.shape
    quarter = outs[0].shape[0]
    step_rows = min(quarter, 512)
    weights = []
    for at in range(0, count, 2):
        blocks = [coefficient_ref[:, i * width : (i + 1) * width].T for i in range(at, min(at + 2, count))]
        joined = jnp.concatenate(blocks, axis=0) if len(blocks) > 1 else blocks[0]
        weights.append(jnp.concatenate(halves_of(joined), axis=1))
    for target, out_ref in zip(which, outs):
        begin = quarter_places()[target] * quarter
        for step in range(0, quarter, step_rows):
            rows = pl.ds(pl.multiple_of(begin + step, step_rows), step_rows)
            sums = None
            for at, weight in zip(range(0, count, 2), weights):
                blocks = [stored_ref[i, rows, :] for i in range(at, min(at + 2, count))]
                joined = jnp.concatenate(blocks, axis=1) if len(blocks) > 1 else blocks[0]
                high, low = halves_of(joined)
                term = product(high, weight) + product(low, weight)
                sums = term if sums is None else sums + term
            out_ref[step : step + step_rows, :] = sums[:, :width] + sums[:, width:]


def correction(which, stored, coefficient):
    count, rows, width = stored.shape
    quarter = rows // 4
    return pl.pallas_call(
        functools.partial(correction_kernel, which),
        in_specs=in_vmem(2),
        out_specs=in_vmem(len(which)),
        out_shape=[jax.ShapeDtypeStruct((quarter, width), f32)] * len(which),
        compiler_params=limits(24),
        cost_estimate=cost(8 * quarter * width * width * count * len(which), 4 * quarter * width * count),
        name="correction",
    )(stored, coefficient)


def remainder_kernel(first_column, lifted_ref, keep_ref, near_ref, far_ref, coefficient_ref, *refs):
    fresh_refs = refs[:-2]
    out_ref, gram_ref = refs[-2:]
    width = out_ref.shape[1]
    value = lifted_ref[...] - ((keep_ref[...] + near_ref[...]) + far_ref[...])
    for at, ref in enumerate(fresh_refs):
        begin = first_column + at * width
        block = coefficient_ref[:, begin : begin + width]
        value = value - lax.dot_general(
            ref[...], block, (((1,), (1,)), ((), ())), precision=highest, preferred_element_type=f32
        )
    out_ref[...] = value
    gram_ref[...] = jnp.dot(value.T, value, precision=highest, preferred_element_type=f32)


def remainder_part(lifted, keep, near, far, coefficient, fresh, first_column):
    quarter, width = far.shape
    return pl.pallas_call(
        functools.partial(remainder_kernel, first_column),
        in_specs=in_vmem(5 + len(fresh)),
        out_specs=in_vmem(2),
        out_shape=[
            jax.ShapeDtypeStruct((quarter, width), f32),
            jax.ShapeDtypeStruct((width, width), f32),
        ],
        compiler_params=limits(16),
        cost_estimate=cost(12 * quarter * width * width * (len(fresh) + 1), 24 * quarter * width),
        name="remainder",
    )(lifted, keep, near, far, coefficient, *fresh)


def factor_kernel(gram_ref, upper_ref, inverse_ref, work):
    width = gram_ref.shape[0]
    row_at = lax.broadcasted_iota(jnp.int32, (width, width), 0)
    column_at = lax.broadcasted_iota(jnp.int32, (width, width), 1)
    work[:, :width] = gram_ref[...]
    work[:, width:] = (row_at == column_at).astype(f32)
    panel_row = lax.broadcasted_iota(jnp.int32, (PANEL, width), 0)
    panel_column = lax.broadcasted_iota(jnp.int32, (PANEL, width), 1)
    for begin in range(0, width, PANEL):
        end = begin + PANEL
        left = work[begin:end, :width]
        right = work[begin:end, width:]
        columns = [
            jnp.broadcast_to(left[:, begin + at : begin + at + 1], (PANEL, width)) for at in range(PANEL)
        ]
        for at in range(PANEL):
            scale = lax.rsqrt(columns[at][at : at + 1, :])
            column = columns[at] * scale
            below = jnp.where(panel_row > at, column, 0.0)
            left_row = left[at : at + 1, :] * scale
            right_row = right[at : at + 1, :] * scale
            left = jnp.where(panel_row == at, left_row, left - below * left_row)
            right = jnp.where(panel_row == at, right_row, right - below * right_row)
            for other in range(at + 1, PANEL):
                columns[other] = columns[other] - below * column[other : other + 1, :]
        left = jnp.where(panel_column >= panel_row + begin, left, 0.0)
        upper_ref[begin:end, :] = left
        inverse_ref[begin:end, :] = right
        if end < width:
            multipliers = left.T[end:, :]
            work[end:, :] -= jnp.dot(
                multipliers,
                jnp.concatenate([left, right], axis=1),
                precision=highest,
                preferred_element_type=f32,
            )


def factor(gram):
    width = gram.shape[0]
    return pl.pallas_call(
        factor_kernel,
        out_shape=[jax.ShapeDtypeStruct((width, width), f32)] * 2,
        scratch_shapes=[pltpu.VMEM((width, 2 * width), f32)],
        compiler_params=limits(8),
        cost_estimate=cost(2e8, 4 * gram.size),
        name="factor",
    )(gram)


def solve_kernel(count, inverse_ref, *refs):
    joined = jnp.concatenate(halves_of(inverse_ref[...].T), axis=1)
    right = jnp.concatenate([joined, joined], axis=0)
    width = inverse_ref.shape[0]
    for at in range(count):
        value_ref, scale_ref, out_ref, scaled_ref = refs[at::count]
        left = jnp.concatenate(halves_of(value_ref[...]), axis=1)
        sums = product(left, right)
        value = sums[:, :width] + sums[:, width:]
        out_ref[...] = value
        scaled_ref[...] = (scale_ref[...] * value).astype(bf16)


def solve(inverse, values, scales):
    count = len(values)
    quarter, width = values[0].shape
    outs = pl.pallas_call(
        functools.partial(solve_kernel, count),
        in_specs=in_vmem(1 + 2 * count),
        out_specs=in_vmem(2 * count),
        out_shape=[jax.ShapeDtypeStruct((quarter, width), f32)] * count
        + [jax.ShapeDtypeStruct((quarter, width), bf16)] * count,
        compiler_params=limits(16),
        cost_estimate=cost(8 * count * quarter * width * width, 12 * count * quarter * width),
        name="solve",
    )(inverse, *values, *scales)
    return outs[:count], outs[count:]


def put_kernel(place_ref, *refs):
    out_ref = refs[-1]
    for at in range(4):

        @pl.when(pl.program_id(0) == at)
        def _():
            for i, ref in enumerate(refs[at:-1:4]):
                out_ref[i] = ref[...]


def put(place, blocks, total):
    quarter, width = blocks[0][0].shape
    flat = [block for quarters in blocks for block in quarters]
    return pl.pallas_call(
        put_kernel,
        grid_spec=pltpu.PrefetchScalarGridSpec(
            num_scalar_prefetch=1,
            grid=(4,),
            in_specs=[pl.BlockSpec((quarter, width), lambda i, at: (0, 0))] * len(flat),
            out_specs=pl.BlockSpec((len(blocks), quarter, width), lambda i, at: (0, at[i], 0)),
        ),
        out_shape=jax.ShapeDtypeStruct((total, 4 * quarter, width), f32),
        compiler_params=limits(16),
        cost_estimate=cost(1e6, 32 * quarter * width),
        name="put",
    )(place, *flat)


def finish_kernel(steps, blocks_ref, inverse_ref, *refs):
    values, refs = refs[:4], refs[4:]
    coefficient_refs, upper_refs, refs = refs[:steps], refs[steps : 2 * steps], refs[2 * steps :]
    out_ref, diagonal_ref, factor_ref, held, sent = refs
    quarter, width = values[0].shape
    joined = jnp.concatenate(halves_of(inverse_ref[...].T), axis=1)
    right = jnp.concatenate([joined, joined], axis=0)
    copies = []
    for at, place in enumerate(quarter_places()):
        left = jnp.concatenate(halves_of(values[at][...]), axis=1)
        sums = product(left, right)
        held[at] = sums[:, :width] + sums[:, width:]
        rows = pl.ds(pl.multiple_of(place * quarter, quarter), quarter)
        copies.append(pltpu.make_async_copy(held.at[at], out_ref.at[steps - 1, rows], sent.at[at]))
        copies[-1].start()
    for at in range(steps):
        diagonal_ref[at] = coefficient_refs[at][:, -width:].T
        factor_ref[at] = upper_refs[at][...]
    for copy in copies:
        copy.wait()


def finish(blocks, inverse, values, coefficients_list, uppers):
    quarter, width = values[0].shape
    steps = len(uppers)
    small = jax.ShapeDtypeStruct((steps, width, width), f32)
    return pl.pallas_call(
        functools.partial(finish_kernel, steps),
        in_specs=[pl.BlockSpec(memory_space=pl.ANY)] + in_vmem(5 + 2 * steps),
        out_specs=[pl.BlockSpec(memory_space=pl.ANY)] + in_vmem(2),
        out_shape=[jax.ShapeDtypeStruct(blocks.shape, f32), small, small],
        scratch_shapes=[pltpu.VMEM((4, quarter, width), f32), pltpu.SemaphoreType.DMA((4,))],
        input_output_aliases={0: 0},
        compiler_params=limits(16),
        cost_estimate=cost(32 * quarter * width * width, 48 * quarter * width),
        name="finish",
    )(blocks, inverse, *values, *coefficients_list, *uppers)


def along_rows(value, by):
    length = lax.axis_size("rows")
    return lax.ppermute(value, "rows", [(i, (i + by) % length) for i in range(length)])


def across(value, bit):
    return lax.ppermute(value, "basis", [(i, i ^ bit) for i in range(lax.axis_size("basis"))])


def spread_kernel(nodes, taken_ref, out_ref):
    total = taken_ref[0]
    for at in range(1, taken_ref.shape[0]):
        total = total + taken_ref[at]
    total = total / nodes
    for at in range(out_ref.shape[0]):
        out_ref[at] = total


def summed(value, axes, nodes):
    rows, columns = value.shape
    devices = 1
    for axis in axes:
        devices *= lax.axis_size(axis)
    if rows % devices:
        return lax.psum(value, axes) / nodes
    pieces = value.reshape(devices, rows // devices, columns)
    taken = lax.all_to_all(pieces, axes, 0, 0, tiled=True)
    spread = pl.pallas_call(
        functools.partial(spread_kernel, nodes),
        in_specs=in_vmem(1),
        out_specs=in_vmem(1)[0],
        out_shape=jax.ShapeDtypeStruct(pieces.shape, f32),
        compiler_params=limits(8),
        cost_estimate=cost(pieces.size, 8 * pieces.size),
        name="spread",
    )(taken)
    return lax.all_to_all(spread, axes, 0, 0, tiled=True).reshape(rows, columns)


def local(tiles, tile_pairs, degree, start_block, stored):
    rows_count = lax.axis_size("rows")
    rows_index = lax.axis_index("rows")
    local_rows, width = start_block.shape
    first_fresh = stored.shape[0] * width
    quarter = local_rows // 4
    blocks_here = local_rows // tiles.shape[1]
    all_nodes = local_rows * rows_count
    all_blocks = blocks_here * rows_count
    row_local = tile_pairs[:, 0] - rows_index * blocks_here
    column_local = jnp.mod(tile_pairs[:, 1] - (rows_index - REACH) * blocks_here, all_blocks)
    row_scale = jnp.broadcast_to((1.0 / jnp.sqrt(degree.astype(f32)))[:, None], start_block.shape)
    places = quarter_places()

    def quarters_of(value):
        return [lax.dynamic_slice_in_dim(value, place * quarter, quarter, 0) for place in places]

    current = quarters_of(start_block)
    scaled = [(scale * block).astype(bf16) for scale, block in zip(quarters_of(row_scale), current)]
    scales = quarters_of(row_scale)
    scale_half = jnp.concatenate(scales[:2])
    fresh = [current]
    coefficients_list, factor_list = ([], [])
    blocks = None
    for iteration in range(ITERS):
        last = iteration == ITERS - 1
        pieces = {0: [scaled[:2], scaled[2:]]}
        for distance in range(REACH, 0, -1):
            for by in (-distance, distance):
                if distance > 1:
                    own = along_rows(scaled[0], -by)
                    mine = [own, across(own, CHIP_BIT)]
                else:
                    mine = [along_rows(jnp.concatenate(scaled[:2]), -by)]
                pieces[by] = [mine, [across(piece, CORE_BIT) for piece in mine]]
        if last:
            blocks = put(jnp.stack(places), fresh[1:], ITERS)
            row_local, blocks = lax.optimization_barrier((row_local, blocks))
        ranges = [by + REACH for by in pieces]
        sources = list(pieces.values())
        keep, send = tile_products(tiles, row_local, column_local, ranges, sources)
        here = keep + across(send, CORE_BIT)
        there = across(here, CHIP_BIT)
        image = here + jnp.concatenate([there[quarter:], there[:quarter]])
        lifted = jnp.concatenate(current[:2]) - scale_half * image
        lifted_other = across(lifted, CORE_BIT)
        part = coefficients((0, 1), lifted, stored, fresh, None)
        part = coefficients((2, 3), lifted_other, stored, fresh, part)
        lifted_own = lifted[:quarter]
        coefficient = summed(part, ("rows",), all_nodes)
        term_cross, term_far = correction((3, 1), stored, coefficient)
        term_near, term_own = correction((2, 0), stored, coefficient)
        far_sum = across(term_far + across(term_cross, CORE_BIT), CHIP_BIT)
        near_sum = across(term_near, CORE_BIT)
        remainder, gram_part = remainder_part(
            lifted_own, term_own, near_sum, far_sum, coefficient, [block[0] for block in fresh], first_fresh
        )
        remainder_near = across(remainder, CORE_BIT)
        remainder_far = across(remainder, CHIP_BIT)
        gram = summed(gram_part, ("rows", "basis"), all_nodes)
        remainder_far, _ = lax.optimization_barrier((remainder_far, gram))
        remainder_cross = across(remainder_far, CORE_BIT)
        upper, inverse = factor(gram)
        coefficients_list.append(coefficient)
        factor_list.append(upper)
        values = [remainder, remainder_far, remainder_near, remainder_cross]
        if last:
            return tuple(finish(blocks, inverse, values, coefficients_list, factor_list))
        current, scaled = solve(inverse, values, scales)
        fresh.append(current)


def solution(mesh):
    placed = (
        P(("rows", "basis"), None, None),
        P(("rows", "basis"), None),
        P("rows"),
        P("rows", None),
        P("basis", "rows", None),
    )
    return jax.shard_map(
        local,
        mesh=mesh,
        in_specs=placed,
        out_specs=(P(None, "rows", None), P(), P()),
        check_vma=False,
    )
```
